128 devices in a mesh: worker: 16 (over y, z), mp: 8 (over x, core).
Axes of the slice: x: 4, y: 4, z: 4, core: 2. Of those that a mesh axis runs over, the one named last changes fastest.
Arguments:
- gradients: bfloat16 [256, 2097152], P('worker', 'mp'), may hold values from -30 to 30
- center: float32 [2097152], P('mp'), may hold values from -6 to 6
- outside_sq: float32 [3, 256], P(None, 'worker'), may hold values from 419430.4 to 4194304
- radius: float32 [3], replicated, may hold values from 1.5 to 3
Outputs:
- new_center: float32 [2097152], P('mp')
- norms: float32 [256], P('worker')
The draws below stay inside these ranges and needn't reach their ends.
All inputs are finite; a program needn't handle non-finite values.
Results may differ from the reference program's by a relative error of at most 0.0003.
Values sent between devices are 32-bit elements; how exact they have to be, the bound alone decides.
A program may use at most 64 MiB of HBM per device.

```python
import math
import jax
import jax.numpy as jnp
from jax import lax

W_DEV = 16
ITERS = 3
WORKERS = 256
P_SIZE = 2097152


def draw_gradients(key, part):
    first = jax.random.fold_in(key, 11)
    second = jax.random.fold_in(key, 12)
    scales = jnp.exp(jax.random.uniform(first, (WORKERS, 1), jnp.float32, jnp.log(0.3), jnp.log(5.0)))
    values = scales * jnp.clip(jax.random.normal(second, (WORKERS, P_SIZE), jnp.float32), -6.0, 6.0)
    return values.astype(jnp.bfloat16)


def block_scale(rng, extent, shards, smallest, high):
    loudness = 1.0
    for dim, shards_of in shards:
        draws = jax.random.uniform(jax.random.fold_in(jax.random.fold_in(rng, 6), dim), (shards_of,), jnp.float32, smallest / len(shards), high / len(shards))
        loudness = loudness * jnp.repeat(jnp.exp(draws), extent[dim] // shards_of).reshape((-1,) + (1,) * (len(extent) - 1 - dim))
    return loudness


def gaussian(stream_key, dims, width, reach, cuts=(), kind=jnp.bfloat16):
    entries = jax.random.normal(stream_key, dims, jnp.float32) * width
    if len(cuts) > 0:
        entries = block_scale(stream_key, dims, cuts, -0.22, 0.18) * entries
    return jnp.clip(entries, min=-reach, max=reach).astype(kind)


def setup_inputs(seed: int = 0) -> dict:
    seeds = jax.random.split(jax.random.key(seed), 5)
    gradients = draw_gradients(jax.random.fold_in(seeds[4], 71), 0)
    center = gaussian(seeds[1], (P_SIZE,), 1.0, 6.0, ((0, 8),), jnp.float32)
    outside_sq = jnp.clip(419430.4 + 3774873.6 * jax.random.uniform(seeds[2], (ITERS, WORKERS), jnp.float32) ** block_scale(seeds[2], (ITERS, WORKERS), ((1, 16),), -0.2, 0.2), 419430.4, 4194304)
    radius = jnp.clip(jnp.exp(jax.random.uniform(seeds[3], (ITERS,), jnp.float32, math.log(1.5), math.log(3.0))), 1.5, 3.0)
    return dict(gradients=gradients, center=center, outside_sq=outside_sq, radius=radius)


def reference(gradients, center, outside_sq, radius):
    blocks = gradients.reshape(WORKERS // W_DEV, W_DEV, P_SIZE)
    root_total = jnp.sqrt(jnp.float32(P_SIZE))
    value = center
    norms = jnp.zeros((WORKERS,), jnp.float32)
    for step in range(ITERS):

        def squares(block):
            diff = block.astype(jnp.float32) - value[None, :]
            return lax.optimization_barrier(jnp.sum(diff * diff, axis=1))
        partial_value = lax.map(squares, blocks).reshape(WORKERS)
        norms = jnp.sqrt(partial_value + outside_sq[step])
        factor = jnp.minimum(jnp.float32(1.0), radius[step] * root_total / norms)
        factor_blocks = factor.reshape(WORKERS // W_DEV, W_DEV)

        def accumulate(total, pair):
            block, weights = pair
            diff = block.astype(jnp.float32) - value[None, :]
            return (total + lax.optimization_barrier(jnp.sum(weights[:, None] * diff, axis=0)), None)
        summed, unused = lax.scan(accumulate, jnp.zeros((P_SIZE,), jnp.float32), (blocks, factor_blocks))
        value = value + summed / jnp.float32(WORKERS)
    return (value, norms)
```

```python
import jax
import jax.numpy as jnp
from jax import lax
from jax.experimental import pallas as pl
from jax.experimental.pallas import tpu as pltpu
from jax.sharding import PartitionSpec as P

ITERS = 3
SIDE = 4
LANES = 128
TILE = 32
LOADS = 16
MESH = pl.DeviceIdType.MESH


def kernel(
    workers_all, root_total, peers,
    radius_ref, grads_hbm, center_hbm, outside_ref,
    out_ref, norms_ref,
    grads, value, local, first, second, second_out, sums, weights,
    load_sem, center_sem, sum_send, sum_recv,
    first_send, first_recv, second_send, second_recv,
    third_send, third_recv, fourth_send, fourth_recv,
):
    workers = grads.shape[0]
    rows = value.shape[1]
    half_rows = rows // 2
    block = half_rows // (SIDE * SIDE)
    chunk = block * SIDE
    per_load = rows // LOADS
    worker = lax.axis_index("worker")
    part = lax.axis_index("mp")
    at = (lax.div(worker, SIDE), lax.rem(worker, SIDE))

    def turned(place, by):
        return lax.rem(place + by, SIDE)

    def device(half, along, across):
        spots = [None, None]
        spots[half] = turned(at[half], along)
        spots[1 - half] = turned(at[1 - half], across)
        return {"worker": spots[0] * SIDE + spots[1], "mp": part}

    def rows_of(half, along, across):
        start = half * half_rows + turned(at[half], along) * chunk + turned(at[1 - half], across) * block
        return pl.ds(pl.multiple_of(start, block), block)

    def send(src, dst, send_sem, recv_sem, to):
        return pltpu.make_async_remote_copy(
            src_ref=src, dst_ref=dst, send_sem=send_sem, recv_sem=recv_sem,
            device_id=to, device_id_type=MESH,
        )

    center_copy = pltpu.make_async_copy(center_hbm, value.at[0], center_sem)
    center_copy.start()

    def load(i):
        columns = pl.ds(i * per_load * LANES, per_load * LANES)
        return pltpu.make_async_copy(grads_hbm.at[:, columns], grads.at[:, columns], load_sem.at[i])

    for i in range(LOADS):
        load(i).start()

    barrier = pltpu.get_barrier_semaphore()
    greeted = 0
    for half in range(2):
        for by in range(1, SIDE):
            pl.semaphore_signal(barrier, 1, device_id=device(half, by, 0), device_id_type=MESH)
            greeted += 1
    for by in range(1, peers):
        pl.semaphore_signal(
            barrier, 1, device_id={"worker": worker, "mp": lax.rem(part + by, peers)}, device_id_type=MESH
        )
        greeted += 1

    def squares(step, start, count, totals):
        for k in range(count):
            columns = pl.ds(pl.multiple_of((start + k) * LANES, LANES), LANES)
            diff = grads[:, columns].astype(jnp.float32) - value[step, pl.ds(start + k, 1), :]
            totals = (totals[1], totals[0] + diff * diff)
        return totals

    def squares_of(step, start, count, totals):
        return lax.fori_loop(
            0, count // TILE,
            lambda i, t: squares(step, pl.multiple_of(start + i * TILE, TILE), TILE, t), totals,
        )

    zero = jnp.zeros((workers, LANES), jnp.float32)
    totals = (zero, zero)
    center_copy.wait()
    for i in range(LOADS):
        load(i).wait()
        totals = squares_of(0, i * per_load, per_load, totals)

    pl.semaphore_wait(barrier, greeted)

    own_lane = lax.broadcasted_iota(jnp.int32, (workers, LANES), 1) % workers == lax.broadcasted_iota(
        jnp.int32, (workers, LANES), 0
    )
    own_row = lax.broadcasted_iota(
        jnp.int32, (TILE // 2, 2 * LANES), 1
    ) // workers == lax.broadcasted_iota(jnp.int32, (TILE // 2, 2 * LANES), 0)

    def factors(step, totals):
        each = jnp.sum(totals[0] + totals[1], axis=1, keepdims=True)
        mine = jnp.sum(jnp.where(own_lane, each, 0.0), axis=0, keepdims=True)
        sums[step, pl.ds(part, 1), :] = mine
        copies = []
        for by in range(1, peers):
            copies.append(send(
                sums.at[step, pl.ds(part, 1)], sums.at[step, pl.ds(part, 1)],
                sum_send.at[step, by - 1], sum_recv.at[step, by - 1],
                {"worker": worker, "mp": lax.rem(part + by, peers)},
            ))
        for copy in copies:
            copy.start()
        for copy in copies:
            copy.wait_recv()
        norms = jnp.sqrt(jnp.sum(sums[step], axis=0, keepdims=True) + outside_ref[step : step + 1, :])
        factor = jnp.minimum(1.0, radius_ref[step] * root_total / norms)
        high = factor.astype(jnp.bfloat16).astype(jnp.float32)
        low = (factor - high).astype(jnp.bfloat16).astype(jnp.float32)
        for i, term in enumerate((high, low)):
            wide = jnp.broadcast_to(jnp.concatenate([term, term], axis=1), own_row.shape)
            weights[i * (TILE // 2) : (i + 1) * (TILE // 2), :] = jnp.where(own_row, wide, 0.0).astype(jnp.bfloat16)
        whole = jnp.sum(high + low, axis=1, keepdims=True) * (workers / LANES)
        return norms, whole, copies

    def weigh(step, start, whole):
        for i in range(block // TILE):
            base = pl.multiple_of(start + i * TILE, TILE)
            stacks = []
            for side in range(2):
                stacks.append(jnp.concatenate([
                    grads[:, pl.ds(pl.multiple_of((base + side * (TILE // 2) + j) * LANES, LANES), LANES)]
                    for j in range(TILE // 2)
                ], axis=0))
            both = jnp.dot(weights[...], jnp.concatenate(stacks, axis=1), preferred_element_type=jnp.float32)
            both = both[: TILE // 2] + both[TILE // 2 :]
            for side in range(2):
                here = pl.ds(pl.multiple_of(base + side * (TILE // 2), TILE // 2), TILE // 2)
                local[here, :] = both[:, side * LANES : (side + 1) * LANES] - whole * value[step, here, :]

    order = (1, 2, 3, 0)
    reach = (2, 1, 3)

    for step in range(ITERS):
        norms, whole, pending = factors(step, totals)
        if step == ITERS - 1:
            norms_ref[...] = norms

        def first_copy(half, along, across):
            here = rows_of(half, along, across)
            at_start = pl.multiple_of(turned(at[1 - half], across) * block, block)
            return send(
                local.at[here], first.at[step, half, along - 1, pl.ds(at_start, block)],
                first_send.at[half, along - 1, across], first_recv.at[step, half, along - 1, across],
                device(half, along, 0),
            )

        def spread(i, carry):
            across = lax.rem(i + 1, SIDE)
            for along in reach + (0,):
                for half in range(2):
                    here = rows_of(half, along, across)
                    weigh(step, here.start, whole)
                    if along:
                        first_copy(half, along, across).start()
            return carry

        lax.fori_loop(0, SIDE, spread, 0)

        def second_copy(half, across):
            return send(
                second_out.at[half, across - 1], second.at[step, half, across - 1],
                second_send.at[half, across - 1], second_recv.at[step, half, across - 1],
                device(half, 0, across),
            )

        kept = [None, None]
        for across in order:
            for half in range(2):
                at_start = pl.multiple_of(turned(at[1 - half], across) * block, block)
                total = local[rows_of(half, 0, across), :]
                for along in range(1, SIDE):
                    first_copy(half, along, across).wait_recv()
                    total = total + first[step, half, along - 1, pl.ds(at_start, block), :]
                if across:
                    second_out[half, across - 1] = total
                    second_copy(half, across).start()
                else:
                    local[rows_of(half, 0, 0), :] = total

        def third_copy(half, across):
            here = rows_of(half, 0, 0)
            return send(
                value.at[step + 1, here], value.at[step + 1, here],
                third_send.at[half, across - 1], third_recv.at[step, half, across - 1],
                device(half, 0, across),
            )

        def fourth_copy(half, along, across):
            here = rows_of(half, 0, SIDE - across)
            return send(
                value.at[step + 1, here], value.at[step + 1, here],
                fourth_send.at[half, along - 1, across], fourth_recv.at[step, half, along - 1, across],
                device(half, along, 0),
            )

        for half in range(2):
            here = rows_of(half, 0, 0)
            total = local[here, :]
            for across in range(1, SIDE):
                second_copy(half, across).wait_recv()
                total = total + second[step, half, across - 1]
            value[step + 1, here, :] = value[step, here, :] + total / workers_all
            for across in reach:
                third_copy(half, across).start()
            for along in reach:
                fourth_copy(half, along, 0).start()

        totals = (zero, zero)

        def taken(half, along, across, totals):
            if step == ITERS - 1:
                return totals
            return squares_of(step + 1, rows_of(half, along, across).start, block, totals)

        for half in range(2):
            totals = taken(half, 0, 0, totals)
        for across in (1, 3, 2):
            for half in range(2):
                third_copy(half, across).wait_recv()
                for along in reach:
                    fourth_copy(half, along, across).start()
                totals = taken(half, 0, SIDE - across, totals)
        for across in (0, 1, 3, 2):
            for along in (1, 3, 2):
                for half in range(2):
                    fourth_copy(half, along, across).wait_recv()
                    totals = taken(half, SIDE - along, SIDE - across, totals)

        for copy in pending:
            copy.wait_send()
        for half in range(2):
            for across in range(SIDE):
                for along in range(1, SIDE):
                    first_copy(half, along, across).wait_send()
                    fourth_copy(half, along, across).wait_send()
            for across in range(1, SIDE):
                second_copy(half, across).wait_send()
                third_copy(half, across).wait_send()

    out_ref[...] = value[ITERS]


def shards(gradients, center, outside_sq, radius):
    workers, length = gradients.shape
    rows = length // LANES
    peers = lax.axis_size("mp")
    workers_all = workers * lax.axis_size("worker")
    root_total = float(length * peers) ** 0.5
    half_rows = rows // 2
    block = half_rows // (SIDE * SIDE)
    chunk = block * SIDE

    def body(*refs):
        kernel(float(workers_all), root_total, peers, *refs)

    dma = pltpu.SemaphoreType.DMA
    center_out, norms = pl.pallas_call(
        body,
        out_shape=(
            jax.ShapeDtypeStruct((rows, LANES), jnp.float32),
            jax.ShapeDtypeStruct((1, LANES), jnp.float32),
        ),
        in_specs=[
            pl.BlockSpec(memory_space=pltpu.SMEM),
            pl.BlockSpec(memory_space=pl.ANY),
            pl.BlockSpec(memory_space=pl.ANY),
            pl.BlockSpec(memory_space=pltpu.VMEM),
        ],
        out_specs=(pl.BlockSpec(memory_space=pltpu.VMEM), pl.BlockSpec(memory_space=pltpu.VMEM)),
        scratch_shapes=[
            pltpu.VMEM((workers, length), jnp.bfloat16),
            pltpu.VMEM((ITERS + 1, rows, LANES), jnp.float32),
            pltpu.VMEM((rows, LANES), jnp.float32),
            pltpu.VMEM((ITERS, 2, SIDE - 1, chunk, LANES), jnp.float32),
            pltpu.VMEM((ITERS, 2, SIDE - 1, block, LANES), jnp.float32),
            pltpu.VMEM((2, SIDE - 1, block, LANES), jnp.float32),
            pltpu.VMEM((ITERS, peers, LANES), jnp.float32),
            pltpu.VMEM((TILE, 2 * LANES), jnp.bfloat16),
            dma((LOADS,)),
            dma(()),
            dma((ITERS, peers - 1)),
            dma((ITERS, peers - 1)),
            dma((2, SIDE - 1, SIDE)),
            dma((ITERS, 2, SIDE - 1, SIDE)),
            dma((2, SIDE - 1)),
            dma((ITERS, 2, SIDE - 1)),
            dma((2, SIDE - 1)),
            dma((ITERS, 2, SIDE - 1)),
            dma((2, SIDE - 1, SIDE)),
            dma((ITERS, 2, SIDE - 1, SIDE)),
        ],
        compiler_params=pltpu.CompilerParams(
            collective_id=0, has_side_effects=True, vmem_limit_bytes=48 * 1024 * 1024
        ),
    )(
        radius,
        gradients,
        center.reshape(rows, LANES),
        jnp.tile(outside_sq, (1, LANES // workers)),
    )
    return center_out.reshape(length), norms[0, :workers]


def solution(mesh):
    placed = (P("worker", "mp"), P("mp"), P(None, "worker"), P())
    return jax.shard_map(
        shards, mesh=mesh, in_specs=placed, out_specs=(P("mp"), P("worker")), check_vma=False
    )
```

```python
import jax
import jax.numpy as jnp
from jax import lax
from jax.experimental import pallas as pl
from jax.experimental.pallas import tpu as pltpu
from jax.sharding import PartitionSpec as P

ITERS = 3
SIDE = 4
LANES = 128
GROUPS = 2
LOADS = 16
MESH = pl.DeviceIdType.MESH


def kernel(
    workers_all, root_total, peers,
    radius_hbm, grads_hbm, center_hbm, outside_hbm,
    out_ref, norms_ref,
    radius, outside, grads, value, local, first, second, second_out, sums, weights,
    small_sem, load_sem, center_sem, sum_send, sum_recv,
    first_send, first_recv, second_send, second_recv,
    third_send, third_recv, fourth_send, fourth_recv,
):
    workers = grads.shape[0]
    rows = value.shape[1]
    half_rows = rows // 2
    block = half_rows // (SIDE * SIDE)
    chunk = block * SIDE
    sub = block // GROUPS
    stacks = sub // workers
    per_load = rows // LOADS
    worker = lax.axis_index("worker")
    part = lax.axis_index("mp")
    at = (lax.div(worker, SIDE), lax.rem(worker, SIDE))

    def turned(place, by):
        return lax.rem(place + by, SIDE)

    def device(half, along, across):
        spots = [None, None]
        spots[half] = turned(at[half], along)
        spots[1 - half] = turned(at[1 - half], across)
        return {"worker": spots[0] * SIDE + spots[1], "mp": part}

    def rows_of(half, along, across, group):
        start = half * half_rows + turned(at[half], along) * chunk + turned(at[1 - half], across) * block
        return pl.ds(pl.multiple_of(start + group * sub, sub), sub)

    def send(src, dst, send_sem, recv_sem, to):
        return pltpu.make_async_remote_copy(
            src_ref=src, dst_ref=dst, send_sem=send_sem, recv_sem=recv_sem,
            device_id=to, device_id_type=MESH,
        )

    def load(i):
        here = pl.ds(i * per_load, per_load)
        columns = pl.ds(i * per_load * LANES, per_load * LANES)
        return (
            pltpu.make_async_copy(center_hbm.at[here], value.at[0, here], center_sem.at[i]),
            pltpu.make_async_copy(grads_hbm.at[:, columns], grads.at[:, columns], load_sem.at[i]),
        )

    for i in range(LOADS):
        for copy in load(i):
            copy.start()
    small = (
        pltpu.make_async_copy(radius_hbm, radius, small_sem.at[0]),
        pltpu.make_async_copy(outside_hbm, outside, small_sem.at[1]),
    )
    for copy in small:
        copy.start()

    barrier = pltpu.get_barrier_semaphore()
    greeted = 0
    for half in range(2):
        for by in range(1, SIDE):
            pl.semaphore_signal(barrier, 1, device_id=device(half, by, 0), device_id_type=MESH)
            greeted += 1
    for by in range(1, peers):
        pl.semaphore_signal(
            barrier, 1, device_id={"worker": worker, "mp": lax.rem(part + by, peers)}, device_id_type=MESH
        )
        greeted += 1

    def squares(step, start, count, totals):
        for k in range(count):
            columns = pl.ds(pl.multiple_of((start + k) * LANES, LANES), LANES)
            diff = grads[:, columns].astype(jnp.float32) - value[step, pl.ds(start + k, 1), :]
            totals = (totals[1], totals[0] + diff * diff)
        return totals

    def squares_of(step, start, count, totals):
        return lax.fori_loop(
            0, count // 32,
            lambda i, t: squares(step, pl.multiple_of(start + i * 32, 32), 32, t), totals,
        ) if count > 32 else squares(step, start, count, totals)

    own_lane = lax.broadcasted_iota(jnp.int32, (workers, LANES), 1) % workers == lax.broadcasted_iota(
        jnp.int32, (workers, LANES), 0
    )
    own_row = lax.broadcasted_iota(
        jnp.int32, (workers, 2 * LANES), 1
    ) // workers == lax.broadcasted_iota(jnp.int32, (workers, 2 * LANES), 0)

    zero = jnp.zeros((workers, LANES), jnp.float32)
    totals = (zero, zero)
    for i in range(LOADS):
        for copy in load(i):
            copy.wait()
        totals = squares_of(0, i * per_load, per_load, totals)
    for copy in small:
        copy.wait()
    elsewhere = jnp.concatenate([outside[...]] * (LANES // workers), axis=1)

    pl.semaphore_wait(barrier, greeted)

    def factors(step, totals, pending):
        each = jnp.sum(totals[0] + totals[1], axis=1, keepdims=True)
        mine = jnp.sum(jnp.where(own_lane, each, 0.0), axis=0, keepdims=True)
        sums[step, pl.ds(part, 1), :] = mine
        copies = []
        for by in range(1, peers):
            copies.append(send(
                sums.at[step, pl.ds(part, 1)], sums.at[step, pl.ds(part, 1)],
                sum_send.at[step, by - 1], sum_recv.at[step, by - 1],
                {"worker": worker, "mp": lax.rem(part + by, peers)},
            ))
        for copy in copies:
            copy.start()
        for copy in pending:
            copy.wait_send()
        for copy in copies:
            copy.wait_recv()
        norms = jnp.sqrt(jnp.sum(sums[step], axis=0, keepdims=True) + elsewhere[step : step + 1, :])
        factor = jnp.minimum(1.0, radius[step] * root_total / norms)
        high = factor.astype(jnp.bfloat16).astype(jnp.float32)
        low = (factor - high).astype(jnp.bfloat16).astype(jnp.float32)
        for i, term in enumerate((high, low)):
            wide = jnp.broadcast_to(jnp.concatenate([term, term], axis=1), own_row.shape)
            weights[i * workers : (i + 1) * workers, :] = jnp.where(own_row, wide, 0.0).astype(jnp.bfloat16)
        whole = jnp.sum(high + low, axis=1, keepdims=True) * (workers / LANES)
        return norms, whole, copies

    def weigh(step, start, whole):
        columns = []
        for i in range(stacks):
            columns.append(jnp.concatenate([
                grads[:, pl.ds(pl.multiple_of((start + i * workers + j) * LANES, LANES), LANES)]
                for j in range(workers)
            ], axis=0))
        both = jnp.dot(weights[...], jnp.concatenate(columns, axis=1), preferred_element_type=jnp.float32)
        both = both[:workers] + both[workers:]
        for i in range(stacks):
            here = pl.ds(pl.multiple_of(start + i * workers, workers), workers)
            local[here, :] = both[:, i * LANES : (i + 1) * LANES] - whole * value[step, here, :]

    reach = (2, 1, 3)

    pending = []
    for step in range(ITERS):
        norms, whole, pending = factors(step, totals, pending)
        if step == ITERS - 1:
            norms_ref[...] = norms

        def first_copy(half, along, across, group):
            here = rows_of(half, along, across, group)
            at_start = pl.multiple_of(turned(at[1 - half], across) * block + group * sub, sub)
            return send(
                local.at[here], first.at[step, half, along - 1, pl.ds(at_start, sub)],
                first_send.at[half, along - 1, across, group], first_recv.at[step, half, along - 1, across, group],
                device(half, along, 0),
            )

        def spread(across, group):
            for along in reach + (0,):
                for half in range(2):
                    weigh(step, rows_of(half, along, across, group).start, whole)
            for along in reach:
                for half in range(2):
                    first_copy(half, along, across, group).start()

        def spread_far(i, carry):
            spread(1 + lax.rem(i, SIDE - 1), lax.div(i, SIDE - 1))
            return carry

        def spread_near(i, carry):
            spread(0, i)
            return carry

        lax.fori_loop(0, (SIDE - 1) * GROUPS, spread_far, 0)
        lax.fori_loop(0, GROUPS, spread_near, 0)

        def second_copy(half, across, group):
            return send(
                second_out.at[half, across - 1, group], second.at[step, half, across - 1, group],
                second_send.at[half, across - 1, group], second_recv.at[step, half, across - 1, group],
                device(half, 0, across),
            )

        def summed(half, across, group):
            at_start = pl.multiple_of(turned(at[1 - half], across) * block + group * sub, sub)
            total = local[rows_of(half, 0, across, group), :]
            for along in reach:
                first_copy(half, along, across, group).wait_recv()
                total = total + first[step, half, along - 1, pl.ds(at_start, sub), :]
            return total

        def third_copy(half, across, group):
            here = rows_of(half, 0, 0, group)
            return send(
                value.at[step + 1, here], value.at[step + 1, here],
                third_send.at[half, across - 1, group], third_recv.at[step, half, across - 1, group],
                device(half, 0, across),
            )

        def fourth_copy(half, along, across, group):
            here = rows_of(half, 0, SIDE - across, group)
            return send(
                value.at[step + 1, here], value.at[step + 1, here],
                fourth_send.at[half, along - 1, across, group], fourth_recv.at[step, half, along - 1, across, group],
                device(half, along, 0),
            )

        for group in range(GROUPS):
            for across in range(1, SIDE):
                for half in range(2):
                    second_out[half, across - 1, group] = summed(half, across, group)
                    second_copy(half, across, group).start()

        for group in range(GROUPS):
            for half in range(2):
                here = rows_of(half, 0, 0, group)
                total = summed(half, 0, group)
                for across in range(1, SIDE):
                    second_copy(half, across, group).wait_recv()
                    total = total + second[step, half, across - 1, group]
                value[step + 1, here, :] = value[step, here, :] + total / workers_all
                for across in reach:
                    third_copy(half, across, group).start()
                for along in reach:
                    fourth_copy(half, along, 0, group).start()

        totals = (zero, zero)

        def taken(half, along, across, group, totals):
            if step == ITERS - 1:
                return totals
            return squares_of(step + 1, rows_of(half, along, across, group).start, sub, totals)

        for group in range(GROUPS):
            for half in range(2):
                totals = taken(half, 0, 0, group, totals)
        for group in range(GROUPS):
            for across in (1, 3, 2):
                for half in range(2):
                    third_copy(half, across, group).wait_recv()
                    for along in reach:
                        fourth_copy(half, along, across, group).start()
                    totals = taken(half, 0, SIDE - across, group, totals)
        for group in range(GROUPS):
            for across in (0, 1, 3, 2):
                for along in (1, 3, 2):
                    for half in range(2):
                        fourth_copy(half, along, across, group).wait_recv()
                        totals = taken(half, SIDE - along, SIDE - across, group, totals)

        pending += [
            copy
            for group in range(GROUPS)
            for half in range(2)
            for copy in [
                make(half, along, across, group)
                for make in (first_copy, fourth_copy) for along in range(1, SIDE) for across in range(SIDE)
            ] + [make(half, across, group) for make in (second_copy, third_copy) for across in range(1, SIDE)]
        ]

    for copy in pending:
        copy.wait_send()
    out_ref[...] = value[ITERS]


def shards(gradients, center, outside_sq, radius):
    workers, length = gradients.shape
    rows = length // LANES
    peers = lax.axis_size("mp")
    workers_all = workers * lax.axis_size("worker")
    root_total = float(length * peers) ** 0.5
    half_rows = rows // 2
    block = half_rows // (SIDE * SIDE)
    chunk = block * SIDE
    sub = block // GROUPS

    def body(*refs):
        kernel(float(workers_all), root_total, peers, *refs)

    dma = pltpu.SemaphoreType.DMA
    center_out, norms = pl.pallas_call(
        body,
        out_shape=(
            jax.ShapeDtypeStruct((rows, LANES), jnp.float32),
            jax.ShapeDtypeStruct((1, LANES), jnp.float32),
        ),
        in_specs=[
            pl.BlockSpec(memory_space=pltpu.HBM),
            pl.BlockSpec(memory_space=pltpu.HBM),
            pl.BlockSpec(memory_space=pltpu.HBM),
            pl.BlockSpec(memory_space=pltpu.HBM),
        ],
        out_specs=(pl.BlockSpec(memory_space=pltpu.VMEM), pl.BlockSpec(memory_space=pltpu.VMEM)),
        scratch_shapes=[
            pltpu.SMEM((ITERS,), jnp.float32),
            pltpu.VMEM((ITERS, workers), jnp.float32),
            pltpu.VMEM((workers, length), jnp.bfloat16),
            pltpu.VMEM((ITERS + 1, rows, LANES), jnp.float32),
            pltpu.VMEM((rows, LANES), jnp.float32),
            pltpu.VMEM((ITERS, 2, SIDE - 1, chunk, LANES), jnp.float32),
            pltpu.VMEM((ITERS, 2, SIDE - 1, GROUPS, sub, LANES), jnp.float32),
            pltpu.VMEM((2, SIDE - 1, GROUPS, sub, LANES), jnp.float32),
            pltpu.VMEM((ITERS, peers, LANES), jnp.float32),
            pltpu.VMEM((2 * workers, 2 * LANES), jnp.bfloat16),
            dma((2,)),
            dma((LOADS,)),
            dma((LOADS,)),
            dma((ITERS, peers - 1)),
            dma((ITERS, peers - 1)),
            dma((2, SIDE - 1, SIDE, GROUPS)),
            dma((ITERS, 2, SIDE - 1, SIDE, GROUPS)),
            dma((2, SIDE - 1, GROUPS)),
            dma((ITERS, 2, SIDE - 1, GROUPS)),
            dma((2, SIDE - 1, GROUPS)),
            dma((ITERS, 2, SIDE - 1, GROUPS)),
            dma((2, SIDE - 1, SIDE, GROUPS)),
            dma((ITERS, 2, SIDE - 1, SIDE, GROUPS)),
        ],
        compiler_params=pltpu.CompilerParams(
            collective_id=0, has_side_effects=True, vmem_limit_bytes=48 * 1024 * 1024
        ),
    )(*(
        pltpu.with_memory_space_constraint(value, pltpu.HBM)
        for value in (radius, gradients, center.reshape(rows, LANES), outside_sq)
    ))
    return center_out.reshape(length), norms[0, :workers]


def solution(mesh):
    placed = (P("worker", "mp"), P("mp"), P(None, "worker"), P())
    return jax.shard_map(
        shards, mesh=mesh, in_specs=placed, out_specs=(P("mp"), P("worker")), check_vma=False
    )
```

```python
import jax
import jax.numpy as jnp
from jax import lax
from jax.experimental import pallas as pl
from jax.experimental.pallas import tpu as pltpu
from jax.sharding import PartitionSpec as P

ITERS = 3
SIDE = 4
LANES = 128
GROUPS = 2
LOADS = 16
MESH = pl.DeviceIdType.MESH


def kernel(
    workers_all, root_total, peers,
    radius_hbm, grads_hbm, center_hbm, outside_hbm,
    out_ref, norms_ref,
    radius, outside, grads, value, local, first, second, second_out, sums, weights,
    small_sem, load_sem, center_sem, sum_send, sum_recv,
    first_send, first_recv, second_send, second_recv,
    third_send, third_recv, fourth_send, fourth_recv,
):
    workers = grads.shape[0]
    rows = value.shape[1]
    half_rows = rows // 2
    block = half_rows // (SIDE * SIDE)
    chunk = block * SIDE
    sub = block // GROUPS
    stacks = sub // workers
    per_load = rows // LOADS
    worker = lax.axis_index("worker")
    part = lax.axis_index("mp")
    at = (lax.div(worker, SIDE), lax.rem(worker, SIDE))

    def turned(place, by):
        return lax.rem(place + by, SIDE)

    def device(half, along, across):
        spots = [None, None]
        spots[half] = turned(at[half], along)
        spots[1 - half] = turned(at[1 - half], across)
        return {"worker": spots[0] * SIDE + spots[1], "mp": part}

    def rows_of(half, along, across, group):
        start = half * half_rows + turned(at[half], along) * chunk + turned(at[1 - half], across) * block
        return pl.ds(pl.multiple_of(start + group * sub, sub), sub)

    def send(src, dst, send_sem, recv_sem, to):
        return pltpu.make_async_remote_copy(
            src_ref=src, dst_ref=dst, send_sem=send_sem, recv_sem=recv_sem,
            device_id=to, device_id_type=MESH,
        )

    def load(i):
        here = pl.ds(i * per_load, per_load)
        columns = pl.ds(i * per_load * LANES, per_load * LANES)
        return (
            pltpu.make_async_copy(center_hbm.at[here], value.at[0, here], center_sem.at[i]),
            pltpu.make_async_copy(grads_hbm.at[:, columns], grads.at[:, columns], load_sem.at[i]),
        )

    for i in range(LOADS):
        for copy in load(i):
            copy.start()
    small = (
        pltpu.make_async_copy(radius_hbm, radius, small_sem.at[0]),
        pltpu.make_async_copy(outside_hbm, outside, small_sem.at[1]),
    )
    for copy in small:
        copy.start()

    barrier = pltpu.get_barrier_semaphore()
    greeted = 0
    for half in range(2):
        for by in range(1, SIDE):
            pl.semaphore_signal(barrier, 1, device_id=device(half, by, 0), device_id_type=MESH)
            greeted += 1
    for by in range(1, peers):
        pl.semaphore_signal(
            barrier, 1, device_id={"worker": worker, "mp": lax.rem(part + by, peers)}, device_id_type=MESH
        )
        greeted += 1

    def squares(step, start, count, totals):
        slab = grads[:, pl.ds(pl.multiple_of(start * LANES, count * LANES), count * LANES)]
        for k in range(count):
            diff = slab[:, k * LANES : (k + 1) * LANES].astype(jnp.float32) - value[step, pl.ds(start + k, 1), :]
            totals = (totals[1], totals[0] + diff * diff)
        return totals

    def squares_of(step, start, count, totals):
        return lax.fori_loop(
            0, count // 32,
            lambda i, t: squares(step, pl.multiple_of(start + i * 32, 32), 32, t), totals,
        ) if count > 32 else squares(step, start, count, totals)

    own_lane = lax.broadcasted_iota(jnp.int32, (workers, LANES), 1) % workers == lax.broadcasted_iota(
        jnp.int32, (workers, LANES), 0
    )
    own_row = lax.broadcasted_iota(
        jnp.int32, (workers, 2 * LANES), 1
    ) // workers == lax.broadcasted_iota(jnp.int32, (workers, 2 * LANES), 0)

    zero = jnp.zeros((workers, LANES), jnp.float32)
    totals = (zero, zero)
    for i in range(LOADS):
        for copy in load(i):
            copy.wait()
        totals = squares_of(0, i * per_load, per_load, totals)
    for copy in small:
        copy.wait()
    elsewhere = jnp.concatenate([outside[...]] * (LANES // workers), axis=1)

    pl.semaphore_wait(barrier, greeted)

    def factors(step, totals, pending):
        each = jnp.sum(totals[0] + totals[1], axis=1, keepdims=True)
        mine = jnp.sum(jnp.where(own_lane, each, 0.0), axis=0, keepdims=True)
        sums[step, pl.ds(part, 1), :] = mine
        copies = []
        for by in range(1, peers):
            copies.append(send(
                sums.at[step, pl.ds(part, 1)], sums.at[step, pl.ds(part, 1)],
                sum_send.at[step, by - 1], sum_recv.at[step, by - 1],
                {"worker": worker, "mp": lax.rem(part + by, peers)},
            ))
        for copy in copies:
            copy.start()
        for copy in pending:
            copy.wait_send()
        for copy in copies:
            copy.wait_recv()
        norms = jnp.sqrt(jnp.sum(sums[step], axis=0, keepdims=True) + elsewhere[step : step + 1, :])
        factor = jnp.minimum(1.0, radius[step] * root_total / norms)
        high = factor.astype(jnp.bfloat16).astype(jnp.float32)
        low = (factor - high).astype(jnp.bfloat16).astype(jnp.float32)
        for i, term in enumerate((high, low)):
            wide = jnp.broadcast_to(jnp.concatenate([term, term], axis=1), own_row.shape)
            weights[i * workers : (i + 1) * workers, :] = jnp.where(own_row, wide, 0.0).astype(jnp.bfloat16)
        whole = jnp.sum(high + low, axis=1, keepdims=True) * (workers / LANES)
        return norms, whole, copies

    def weigh(step, start, whole):
        slab = grads[:, pl.ds(pl.multiple_of(start * LANES, sub * LANES), sub * LANES)]
        columns = []
        for i in range(stacks):
            columns.append(jnp.concatenate([
                slab[:, (i * workers + j) * LANES : (i * workers + j + 1) * LANES] for j in range(workers)
            ], axis=0))
        both = jnp.dot(weights[...], jnp.concatenate(columns, axis=1), preferred_element_type=jnp.float32)
        both = both[:workers] + both[workers:]
        for i in range(stacks):
            here = pl.ds(pl.multiple_of(start + i * workers, workers), workers)
            local[here, :] = both[:, i * LANES : (i + 1) * LANES] - whole * value[step, here, :]

    reach = (2, 1, 3)

    pending = []
    for step in range(ITERS):
        norms, whole, pending = factors(step, totals, pending)
        if step == ITERS - 1:
            norms_ref[...] = norms[0, :workers]

        def first_copy(half, along, across, group):
            here = rows_of(half, along, across, group)
            at_start = pl.multiple_of(turned(at[1 - half], across) * block + group * sub, sub)
            return send(
                local.at[here], first.at[step, half, along - 1, pl.ds(at_start, sub)],
                first_send.at[half, along - 1, across, group], first_recv.at[step, half, along - 1, across, group],
                device(half, along, 0),
            )

        def spread(across, group):
            for along in reach + (0,):
                for half in range(2):
                    weigh(step, rows_of(half, along, across, group).start, whole)
            for along in reach:
                for half in range(2):
                    first_copy(half, along, across, group).start()

        def spread_far(i, carry):
            spread(1 + lax.rem(i, SIDE - 1), lax.div(i, SIDE - 1))
            return carry

        def spread_near(i, carry):
            spread(0, i)
            return carry

        lax.fori_loop(0, (SIDE - 1) * GROUPS, spread_far, 0)
        lax.fori_loop(0, GROUPS, spread_near, 0)

        def second_copy(half, across, group):
            return send(
                second_out.at[half, across - 1, group], second.at[step, half, across - 1, group],
                second_send.at[half, across - 1, group], second_recv.at[step, half, across - 1, group],
                device(half, 0, across),
            )

        def summed(half, across, group):
            at_start = pl.multiple_of(turned(at[1 - half], across) * block + group * sub, sub)
            total = local[rows_of(half, 0, across, group), :]
            for along in reach:
                first_copy(half, along, across, group).wait_recv()
                total = total + first[step, half, along - 1, pl.ds(at_start, sub), :]
            return total

        def third_copy(half, across, group):
            here = rows_of(half, 0, 0, group)
            return send(
                value.at[step + 1, here], value.at[step + 1, here],
                third_send.at[half, across - 1, group], third_recv.at[step, half, across - 1, group],
                device(half, 0, across),
            )

        def fourth_copy(half, along, across, group):
            here = rows_of(half, 0, SIDE - across, group)
            return send(
                value.at[step + 1, here], value.at[step + 1, here],
                fourth_send.at[half, along - 1, across, group], fourth_recv.at[step, half, along - 1, across, group],
                device(half, along, 0),
            )

        for group in range(GROUPS):
            for across in range(1, SIDE):
                for half in range(2):
                    second_out[half, across - 1, group] = summed(half, across, group)
                    second_copy(half, across, group).start()

        for group in range(GROUPS):
            for half in range(2):
                here = rows_of(half, 0, 0, group)
                total = summed(half, 0, group)
                for across in range(1, SIDE):
                    second_copy(half, across, group).wait_recv()
                    total = total + second[step, half, across - 1, group]
                value[step + 1, here, :] = value[step, here, :] + total / workers_all
                for across in reach:
                    third_copy(half, across, group).start()
                for along in reach:
                    fourth_copy(half, along, 0, group).start()

        totals = (zero, zero)

        def taken(half, along, across, group, totals):
            if step == ITERS - 1:
                return totals
            return squares_of(step + 1, rows_of(half, along, across, group).start, sub, totals)

        for group in range(GROUPS):
            for half in range(2):
                totals = taken(half, 0, 0, group, totals)
        for group in range(GROUPS):
            for across in (1, 3, 2):
                for half in range(2):
                    third_copy(half, across, group).wait_recv()
                    for along in reach:
                        fourth_copy(half, along, across, group).start()
                    totals = taken(half, 0, SIDE - across, group, totals)
        for group in range(GROUPS):
            for across in (0, 1, 3, 2):
                for along in (1, 3, 2):
                    for half in range(2):
                        fourth_copy(half, along, across, group).wait_recv()
                        totals = taken(half, SIDE - along, SIDE - across, group, totals)

        pending += [
            copy
            for group in range(GROUPS)
            for half in range(2)
            for copy in [
                make(half, along, across, group)
                for make in (first_copy, fourth_copy) for along in range(1, SIDE) for across in range(SIDE)
            ] + [make(half, across, group) for make in (second_copy, third_copy) for across in range(1, SIDE)]
        ]

    for copy in pending:
        copy.wait_send()
    out_ref[...] = value[ITERS]


def write_out(center_ref, norms_ref, center_out, norms_out, sem):
    copies = (
        pltpu.make_async_copy(center_ref, center_out, sem.at[0]),
        pltpu.make_async_copy(norms_ref, norms_out, sem.at[1]),
    )
    for copy in copies:
        copy.start()
    for copy in copies:
        copy.wait()


def shards(gradients, center, outside_sq, radius):
    workers, length = gradients.shape
    rows = length // LANES
    peers = lax.axis_size("mp")
    workers_all = workers * lax.axis_size("worker")
    root_total = float(length * peers) ** 0.5
    half_rows = rows // 2
    block = half_rows // (SIDE * SIDE)
    chunk = block * SIDE
    sub = block // GROUPS

    def body(*refs):
        kernel(float(workers_all), root_total, peers, *refs)

    dma = pltpu.SemaphoreType.DMA
    center_out, norms = pl.pallas_call(
        body,
        out_shape=(
            jax.ShapeDtypeStruct((rows, LANES), jnp.float32),
            jax.ShapeDtypeStruct((workers,), jnp.float32),
        ),
        in_specs=[
            pl.BlockSpec(memory_space=pltpu.HBM),
            pl.BlockSpec(memory_space=pltpu.HBM),
            pl.BlockSpec(memory_space=pltpu.HBM),
            pl.BlockSpec(memory_space=pltpu.HBM),
        ],
        out_specs=(pl.BlockSpec(memory_space=pltpu.VMEM), pl.BlockSpec(memory_space=pltpu.VMEM)),
        scratch_shapes=[
            pltpu.SMEM((ITERS,), jnp.float32),
            pltpu.VMEM((ITERS, workers), jnp.float32),
            pltpu.VMEM((workers, length), jnp.bfloat16),
            pltpu.VMEM((ITERS + 1, rows, LANES), jnp.float32),
            pltpu.VMEM((rows, LANES), jnp.float32),
            pltpu.VMEM((ITERS, 2, SIDE - 1, chunk, LANES), jnp.float32),
            pltpu.VMEM((ITERS, 2, SIDE - 1, GROUPS, sub, LANES), jnp.float32),
            pltpu.VMEM((2, SIDE - 1, GROUPS, sub, LANES), jnp.float32),
            pltpu.VMEM((ITERS, peers, LANES), jnp.float32),
            pltpu.VMEM((2 * workers, 2 * LANES), jnp.bfloat16),
            dma((2,)),
            dma((LOADS,)),
            dma((LOADS,)),
            dma((ITERS, peers - 1)),
            dma((ITERS, peers - 1)),
            dma((2, SIDE - 1, SIDE, GROUPS)),
            dma((ITERS, 2, SIDE - 1, SIDE, GROUPS)),
            dma((2, SIDE - 1, GROUPS)),
            dma((ITERS, 2, SIDE - 1, GROUPS)),
            dma((2, SIDE - 1, GROUPS)),
            dma((ITERS, 2, SIDE - 1, GROUPS)),
            dma((2, SIDE - 1, SIDE, GROUPS)),
            dma((ITERS, 2, SIDE - 1, SIDE, GROUPS)),
        ],
        compiler_params=pltpu.CompilerParams(
            collective_id=0, has_side_effects=True, vmem_limit_bytes=48 * 1024 * 1024
        ),
    )(*(
        pltpu.with_memory_space_constraint(value, pltpu.HBM)
        for value in (radius, gradients, center.reshape(rows, LANES), outside_sq)
    ))
    center_out, norms = pl.pallas_call(
        write_out,
        out_shape=(
            jax.ShapeDtypeStruct((rows, LANES), jnp.float32),
            jax.ShapeDtypeStruct((workers,), jnp.float32),
        ),
        in_specs=[pl.BlockSpec(memory_space=pl.ANY)] * 2,
        out_specs=(pl.BlockSpec(memory_space=pltpu.HBM),) * 2,
        scratch_shapes=[dma((2,))],
        compiler_params=pltpu.CompilerParams(vmem_limit_bytes=1024 * 1024),
    )(center_out, norms)
    return center_out.reshape(length), norms


def solution(mesh):
    placed = (P("worker", "mp"), P("mp"), P(None, "worker"), P())
    return jax.shard_map(
        shards, mesh=mesh, in_specs=placed, out_specs=(P("mp"), P("worker")), check_vma=False
    )
```

```python
import jax
import jax.numpy as jnp
from jax import lax
from jax.experimental import pallas as pl
from jax.experimental.pallas import tpu as pltpu
from jax.sharding import PartitionSpec as P

ITERS = 3
FAR = (2, 3, 1)
SIDE = 4
LANES = 128
GROUPS = 2
LOADS = 16
MESH = pl.DeviceIdType.MESH


def kernel(
    workers_all, root_total, peers,
    radius_hbm, grads_hbm, center_hbm, outside_hbm,
    out_ref, norms_ref,
    radius, outside, grads, value, local, first, second, second_out, sums, weights,
    small_sem, load_sem, center_sem, sum_send, sum_recv,
    first_send, first_recv, second_send, second_recv,
    third_send, third_recv, fourth_send, fourth_recv,
):
    workers = grads.shape[0]
    rows = value.shape[1]
    half_rows = rows // 2
    block = half_rows // (SIDE * SIDE)
    chunk = block * SIDE
    sub = block // GROUPS
    stacks = sub // workers
    per_load = rows // LOADS
    worker = lax.axis_index("worker")
    part = lax.axis_index("mp")
    at = (lax.div(worker, SIDE), lax.rem(worker, SIDE))

    def turned(place, by):
        return lax.rem(place + by, SIDE)

    def device(half, along, across):
        spots = [None, None]
        spots[half] = turned(at[half], along)
        spots[1 - half] = turned(at[1 - half], across)
        return {"worker": spots[0] * SIDE + spots[1], "mp": part}

    def rows_of(half, along, across, group):
        start = half * half_rows + turned(at[half], along) * chunk + turned(at[1 - half], across) * block
        return pl.ds(pl.multiple_of(start + group * sub, sub), sub)

    def send(src, dst, send_sem, recv_sem, to):
        return pltpu.make_async_remote_copy(
            src_ref=src, dst_ref=dst, send_sem=send_sem, recv_sem=recv_sem,
            device_id=to, device_id_type=MESH,
        )

    def load(i):
        here = pl.ds(i * per_load, per_load)
        columns = pl.ds(i * per_load * LANES, per_load * LANES)
        return (
            pltpu.make_async_copy(center_hbm.at[here], value.at[0, here], center_sem.at[i]),
            pltpu.make_async_copy(grads_hbm.at[:, columns], grads.at[:, columns], load_sem.at[i]),
        )

    for i in range(LOADS):
        for copy in load(i):
            copy.start()
    small = (
        pltpu.make_async_copy(radius_hbm, radius, small_sem.at[0]),
        pltpu.make_async_copy(outside_hbm, outside, small_sem.at[1]),
    )
    for copy in small:
        copy.start()

    barrier = pltpu.get_barrier_semaphore()
    greeted = 0
    for half in range(2):
        for by in range(1, SIDE):
            pl.semaphore_signal(barrier, 1, device_id=device(half, by, 0), device_id_type=MESH)
            greeted += 1
    for by in range(1, peers):
        pl.semaphore_signal(
            barrier, 1, device_id={"worker": worker, "mp": lax.rem(part + by, peers)}, device_id_type=MESH
        )
        greeted += 1

    def squares(step, start, count, totals):
        slab = grads[:, pl.ds(pl.multiple_of(start * LANES, count * LANES), count * LANES)]
        for k in range(count):
            diff = slab[:, k * LANES : (k + 1) * LANES].astype(jnp.float32) - value[step, pl.ds(start + k, 1), :]
            totals = (totals[1], totals[0] + diff * diff)
        return totals

    def squares_of(step, start, count, totals):
        return lax.fori_loop(
            0, count // 32,
            lambda i, t: squares(step, pl.multiple_of(start + i * 32, 32), 32, t), totals,
        ) if count > 32 else squares(step, start, count, totals)

    own_lane = lax.broadcasted_iota(jnp.int32, (workers, LANES), 1) % workers == lax.broadcasted_iota(
        jnp.int32, (workers, LANES), 0
    )
    own_row = lax.broadcasted_iota(
        jnp.int32, (workers, 2 * LANES), 1
    ) // workers == lax.broadcasted_iota(jnp.int32, (workers, 2 * LANES), 0)

    zero = jnp.zeros((workers, LANES), jnp.float32)
    totals = (zero, zero)
    for i in range(LOADS):
        for copy in load(i):
            copy.wait()
        totals = squares_of(0, i * per_load, per_load, totals)
    for copy in small:
        copy.wait()
    elsewhere = jnp.concatenate([outside[...]] * (LANES // workers), axis=1)

    pl.semaphore_wait(barrier, greeted)

    def factors(step, totals, pending):
        each = jnp.sum(totals[0] + totals[1], axis=1, keepdims=True)
        mine = jnp.sum(jnp.where(own_lane, each, 0.0), axis=0, keepdims=True)
        sums[step, pl.ds(part, 1), :] = mine
        copies = []
        for by in range(1, peers):
            copies.append(send(
                sums.at[step, pl.ds(part, 1)], sums.at[step, pl.ds(part, 1)],
                sum_send.at[step, by - 1], sum_recv.at[step, by - 1],
                {"worker": worker, "mp": lax.rem(part + by, peers)},
            ))
        for copy in copies:
            copy.start()
        for copy in pending:
            copy.wait_send()
        for copy in copies:
            copy.wait_recv()
        norms = jnp.sqrt(jnp.sum(sums[step], axis=0, keepdims=True) + elsewhere[step : step + 1, :])
        factor = jnp.minimum(1.0, radius[step] * root_total / norms)
        high = factor.astype(jnp.bfloat16).astype(jnp.float32)
        low = (factor - high).astype(jnp.bfloat16).astype(jnp.float32)
        for i, term in enumerate((high, low)):
            wide = jnp.broadcast_to(jnp.concatenate([term, term], axis=1), own_row.shape)
            weights[i * workers : (i + 1) * workers, :] = jnp.where(own_row, wide, 0.0).astype(jnp.bfloat16)
        whole = jnp.sum(high + low, axis=1, keepdims=True) * (workers / LANES)
        return norms, whole, copies

    def weigh(step, start, whole):
        slab = grads[:, pl.ds(pl.multiple_of(start * LANES, sub * LANES), sub * LANES)]
        columns = []
        for i in range(stacks):
            columns.append(jnp.concatenate([
                slab[:, (i * workers + j) * LANES : (i * workers + j + 1) * LANES] for j in range(workers)
            ], axis=0))
        both = jnp.dot(weights[...], jnp.concatenate(columns, axis=1), preferred_element_type=jnp.float32)
        both = both[:workers] + both[workers:]
        for i in range(stacks):
            here = pl.ds(pl.multiple_of(start + i * workers, workers), workers)
            local[here, :] = both[:, i * LANES : (i + 1) * LANES] - whole * value[step, here, :]

    reach = (2, 1, 3)

    pending = []
    for step in range(ITERS):
        norms, whole, pending = factors(step, totals, pending)
        if step == ITERS - 1:
            norms_ref[...] = norms[0, :workers]

        def first_copy(half, along, across, group):
            here = rows_of(half, along, across, group)
            at_start = pl.multiple_of(turned(at[1 - half], across) * block + group * sub, sub)
            return send(
                local.at[here], first.at[step, half, along - 1, pl.ds(at_start, sub)],
                first_send.at[half, along - 1, across, group], first_recv.at[step, half, along - 1, across, group],
                device(half, along, 0),
            )

        def spread(across, group):
            for along in reach + (0,):
                for half in range(2):
                    weigh(step, rows_of(half, along, across, group).start, whole)
            for along in reach:
                for half in range(2):
                    first_copy(half, along, across, group).start()

        def spread_far(i, carry):
            spread(1 + lax.rem(i + 1, SIDE - 1), lax.div(i, SIDE - 1))
            return carry

        def spread_near(i, carry):
            spread(0, i)
            return carry

        lax.fori_loop(0, (SIDE - 1) * GROUPS, spread_far, 0)
        lax.fori_loop(0, GROUPS, spread_near, 0)

        def second_copy(half, across, group):
            return send(
                second_out.at[half, across - 1, group], second.at[step, half, across - 1, group],
                second_send.at[half, across - 1, group], second_recv.at[step, half, across - 1, group],
                device(half, 0, across),
            )

        def summed(half, across, group):
            at_start = pl.multiple_of(turned(at[1 - half], across) * block + group * sub, sub)
            total = local[rows_of(half, 0, across, group), :]
            for along in reach:
                first_copy(half, along, across, group).wait_recv()
                total = total + first[step, half, along - 1, pl.ds(at_start, sub), :]
            return total

        def third_copy(half, across, group):
            here = rows_of(half, 0, 0, group)
            return send(
                value.at[step + 1, here], value.at[step + 1, here],
                third_send.at[half, across - 1, group], third_recv.at[step, half, across - 1, group],
                device(half, 0, across),
            )

        def fourth_copy(half, along, across, group):
            here = rows_of(half, 0, SIDE - across, group)
            return send(
                value.at[step + 1, here], value.at[step + 1, here],
                fourth_send.at[half, along - 1, across, group], fourth_recv.at[step, half, along - 1, across, group],
                device(half, along, 0),
            )

        for group in range(GROUPS):
            for across in FAR:
                for half in range(2):
                    second_out[half, across - 1, group] = summed(half, across, group)
                    second_copy(half, across, group).start()

        for group in range(GROUPS):
            for half in range(2):
                here = rows_of(half, 0, 0, group)
                total = summed(half, 0, group)
                for across in range(1, SIDE):
                    second_copy(half, across, group).wait_recv()
                    total = total + second[step, half, across - 1, group]
                value[step + 1, here, :] = value[step, here, :] + total / workers_all
                for across in reach:
                    third_copy(half, across, group).start()
                for along in reach:
                    fourth_copy(half, along, 0, group).start()

        totals = (zero, zero)

        def taken(half, along, across, group, totals):
            if step == ITERS - 1:
                return totals
            return squares_of(step + 1, rows_of(half, along, across, group).start, sub, totals)

        for group in range(GROUPS):
            for half in range(2):
                totals = taken(half, 0, 0, group, totals)
        for group in range(GROUPS):
            for across in (1, 3, 2):
                for half in range(2):
                    third_copy(half, across, group).wait_recv()
                    for along in reach:
                        fourth_copy(half, along, across, group).start()
                    totals = taken(half, 0, SIDE - across, group, totals)
        for group in range(GROUPS):
            for across in (0, 1, 3, 2):
                for along in (1, 3, 2):
                    for half in range(2):
                        fourth_copy(half, along, across, group).wait_recv()
                        totals = taken(half, SIDE - along, SIDE - across, group, totals)

        pending += [
            copy
            for group in range(GROUPS)
            for half in range(2)
            for copy in [
                make(half, along, across, group)
                for make in (first_copy, fourth_copy) for along in range(1, SIDE) for across in range(SIDE)
            ] + [make(half, across, group) for make in (second_copy, third_copy) for across in range(1, SIDE)]
        ]

    for copy in pending:
        copy.wait_send()
    out_ref[...] = value[ITERS]


def write_out(center_ref, norms_ref, center_out, norms_out, sem):
    copies = (
        pltpu.make_async_copy(center_ref, center_out, sem.at[0]),
        pltpu.make_async_copy(norms_ref, norms_out, sem.at[1]),
    )
    for copy in copies:
        copy.start()
    for copy in copies:
        copy.wait()


def shards(gradients, center, outside_sq, radius):
    workers, length = gradients.shape
    rows = length // LANES
    peers = lax.axis_size("mp")
    workers_all = workers * lax.axis_size("worker")
    root_total = float(length * peers) ** 0.5
    half_rows = rows // 2
    block = half_rows // (SIDE * SIDE)
    chunk = block * SIDE
    sub = block // GROUPS

    def body(*refs):
        kernel(float(workers_all), root_total, peers, *refs)

    dma = pltpu.SemaphoreType.DMA
    center_out, norms = pl.pallas_call(
        body,
        out_shape=(
            jax.ShapeDtypeStruct((rows, LANES), jnp.float32),
            jax.ShapeDtypeStruct((workers,), jnp.float32),
        ),
        in_specs=[
            pl.BlockSpec(memory_space=pltpu.HBM),
            pl.BlockSpec(memory_space=pltpu.HBM),
            pl.BlockSpec(memory_space=pltpu.HBM),
            pl.BlockSpec(memory_space=pltpu.HBM),
        ],
        out_specs=(pl.BlockSpec(memory_space=pltpu.VMEM), pl.BlockSpec(memory_space=pltpu.VMEM)),
        scratch_shapes=[
            pltpu.SMEM((ITERS,), jnp.float32),
            pltpu.VMEM((ITERS, workers), jnp.float32),
            pltpu.VMEM((workers, length), jnp.bfloat16),
            pltpu.VMEM((ITERS + 1, rows, LANES), jnp.float32),
            pltpu.VMEM((rows, LANES), jnp.float32),
            pltpu.VMEM((ITERS, 2, SIDE - 1, chunk, LANES), jnp.float32),
            pltpu.VMEM((ITERS, 2, SIDE - 1, GROUPS, sub, LANES), jnp.float32),
            pltpu.VMEM((2, SIDE - 1, GROUPS, sub, LANES), jnp.float32),
            pltpu.VMEM((ITERS, peers, LANES), jnp.float32),
            pltpu.VMEM((2 * workers, 2 * LANES), jnp.bfloat16),
            dma((2,)),
            dma((LOADS,)),
            dma((LOADS,)),
            dma((ITERS, peers - 1)),
            dma((ITERS, peers - 1)),
            dma((2, SIDE - 1, SIDE, GROUPS)),
            dma((ITERS, 2, SIDE - 1, SIDE, GROUPS)),
            dma((2, SIDE - 1, GROUPS)),
            dma((ITERS, 2, SIDE - 1, GROUPS)),
            dma((2, SIDE - 1, GROUPS)),
            dma((ITERS, 2, SIDE - 1, GROUPS)),
            dma((2, SIDE - 1, SIDE, GROUPS)),
            dma((ITERS, 2, SIDE - 1, SIDE, GROUPS)),
        ],
        compiler_params=pltpu.CompilerParams(
            collective_id=0, has_side_effects=True, vmem_limit_bytes=48 * 1024 * 1024
        ),
    )(*(
        pltpu.with_memory_space_constraint(value, pltpu.HBM)
        for value in (radius, gradients, center.reshape(rows, LANES), outside_sq)
    ))
    center_out, norms = pl.pallas_call(
        write_out,
        out_shape=(
            jax.ShapeDtypeStruct((rows, LANES), jnp.float32),
            jax.ShapeDtypeStruct((workers,), jnp.float32),
        ),
        in_specs=[pl.BlockSpec(memory_space=pl.ANY)] * 2,
        out_specs=(pl.BlockSpec(memory_space=pltpu.HBM),) * 2,
        scratch_shapes=[dma((2,))],
        compiler_params=pltpu.CompilerParams(vmem_limit_bytes=1024 * 1024),
    )(center_out, norms)
    return center_out.reshape(length), norms


def solution(mesh):
    placed = (P("worker", "mp"), P("mp"), P(None, "worker"), P())
    return jax.shard_map(
        shards, mesh=mesh, in_specs=placed, out_specs=(P("mp"), P("worker")), check_vma=False
    )
```

```python
import jax
import jax.numpy as jnp
from jax import lax
from jax.experimental import pallas as pl
from jax.experimental.pallas import tpu as pltpu
from jax.sharding import PartitionSpec as P

ITERS = 3
FAR = (2, 3, 1)
SIDE = 4
LANES = 128
GROUPS = 2
LOADS = 16
MESH = pl.DeviceIdType.MESH


def kernel(
    workers_all, root_total, peers,
    radius_hbm, grads_hbm, center_hbm, outside_hbm,
    out_ref, norms_ref,
    radius, outside, grads, value, local, first, second, second_out, sums, weights,
    small_sem, load_sem, center_sem, sum_send, sum_recv,
    first_send, first_recv, second_send, second_recv,
    third_send, third_recv, fourth_send, fourth_recv,
):
    workers = grads.shape[0]
    rows = value.shape[1]
    half_rows = rows // 2
    block = half_rows // (SIDE * SIDE)
    chunk = block * SIDE
    sub = block // GROUPS
    stacks = sub // workers
    per_load = rows // LOADS
    worker = lax.axis_index("worker")
    part = lax.axis_index("mp")
    at = (lax.div(worker, SIDE), lax.rem(worker, SIDE))

    def turned(place, by):
        return lax.rem(place + by, SIDE)

    def device(half, along, across):
        spots = [None, None]
        spots[half] = turned(at[half], along)
        spots[1 - half] = turned(at[1 - half], across)
        return {"worker": spots[0] * SIDE + spots[1], "mp": part}

    def rows_of(half, along, across, group):
        start = half * half_rows + turned(at[half], along) * chunk + turned(at[1 - half], across) * block
        return pl.ds(pl.multiple_of(start + group * sub, sub), sub)

    def send(src, dst, send_sem, recv_sem, to):
        return pltpu.make_async_remote_copy(
            src_ref=src, dst_ref=dst, send_sem=send_sem, recv_sem=recv_sem,
            device_id=to, device_id_type=MESH,
        )

    def load(i):
        here = pl.ds(i * per_load, per_load)
        columns = pl.ds(i * per_load * LANES, per_load * LANES)
        return (
            pltpu.make_async_copy(center_hbm.at[here], value.at[0, here], center_sem.at[i]),
            pltpu.make_async_copy(grads_hbm.at[:, columns], grads.at[:, columns], load_sem.at[i]),
        )

    for i in range(LOADS):
        for copy in load(i):
            copy.start()
    small = (
        pltpu.make_async_copy(radius_hbm, radius, small_sem.at[0]),
        pltpu.make_async_copy(outside_hbm, outside, small_sem.at[1]),
    )
    for copy in small:
        copy.start()

    barrier = pltpu.get_barrier_semaphore()
    greeted = 0
    for half in range(2):
        for by in range(1, SIDE):
            pl.semaphore_signal(barrier, 1, device_id=device(half, by, 0), device_id_type=MESH)
            greeted += 1
    for by in range(1, peers):
        pl.semaphore_signal(
            barrier, 1, device_id={"worker": worker, "mp": lax.rem(part + by, peers)}, device_id_type=MESH
        )
        greeted += 1

    def squares(step, start, count, totals):
        slab = grads[:, pl.ds(pl.multiple_of(start * LANES, count * LANES), count * LANES)]
        for k in range(count):
            diff = slab[:, k * LANES : (k + 1) * LANES].astype(jnp.float32) - value[step, pl.ds(start + k, 1), :]
            totals = (totals[1], totals[0] + diff * diff)
        return totals

    def squares_of(step, start, count, totals):
        return lax.fori_loop(
            0, count // 32,
            lambda i, t: squares(step, pl.multiple_of(start + i * 32, 32), 32, t), totals,
        ) if count > 32 else squares(step, start, count, totals)

    own_lane = lax.broadcasted_iota(jnp.int32, (workers, LANES), 1) % workers == lax.broadcasted_iota(
        jnp.int32, (workers, LANES), 0
    )
    own_row = lax.broadcasted_iota(
        jnp.int32, (workers, 2 * LANES), 1
    ) // workers == lax.broadcasted_iota(jnp.int32, (workers, 2 * LANES), 0)

    zero = jnp.zeros((workers, LANES), jnp.float32)
    totals = (zero, zero)
    for i in range(LOADS):
        for copy in load(i):
            copy.wait()
        totals = squares_of(0, i * per_load, per_load, totals)
    for copy in small:
        copy.wait()
    elsewhere = jnp.concatenate([outside[...]] * (LANES // workers), axis=1)

    pl.semaphore_wait(barrier, greeted)

    def factors(step, totals, pending):
        each = jnp.sum(totals[0] + totals[1], axis=1, keepdims=True)
        mine = jnp.sum(jnp.where(own_lane, each, 0.0), axis=0, keepdims=True)
        sums[step, pl.ds(part, 1), :] = mine
        copies = []
        for by in range(1, peers):
            copies.append(send(
                sums.at[step, pl.ds(part, 1)], sums.at[step, pl.ds(part, 1)],
                sum_send.at[step, by - 1], sum_recv.at[step, by - 1],
                {"worker": worker, "mp": lax.rem(part + by, peers)},
            ))
        for copy in copies:
            copy.start()
        for copy in pending:
            copy.wait_send()
        for copy in copies:
            copy.wait_recv()
        norms = jnp.sqrt(jnp.sum(sums[step], axis=0, keepdims=True) + elsewhere[step : step + 1, :])
        factor = jnp.minimum(1.0, radius[step] * root_total / norms)
        high = factor.astype(jnp.bfloat16).astype(jnp.float32)
        low = (factor - high).astype(jnp.bfloat16).astype(jnp.float32)
        for i, term in enumerate((high, low)):
            wide = jnp.broadcast_to(jnp.concatenate([term, term], axis=1), own_row.shape)
            weights[i * workers : (i + 1) * workers, :] = jnp.where(own_row, wide, 0.0).astype(jnp.bfloat16)
        whole = jnp.sum(high + low, axis=1, keepdims=True) * (workers / LANES)
        return norms, whole, copies

    def weigh(step, start, whole):
        slab = grads[:, pl.ds(pl.multiple_of(start * LANES, sub * LANES), sub * LANES)]
        columns = []
        for i in range(stacks):
            columns.append(jnp.concatenate([
                slab[:, (i * workers + j) * LANES : (i * workers + j + 1) * LANES] for j in range(workers)
            ], axis=0))
        both = jnp.dot(weights[...], jnp.concatenate(columns, axis=1), preferred_element_type=jnp.float32)
        both = both[:workers] + both[workers:]
        for i in range(stacks):
            here = pl.ds(pl.multiple_of(start + i * workers, workers), workers)
            local[here, :] = both[:, i * LANES : (i + 1) * LANES] - whole * value[step, here, :]

    reach = (2, 1, 3)

    pending = []
    for step in range(ITERS):
        norms, whole, pending = factors(step, totals, pending)
        if step == ITERS - 1:
            norms_ref[...] = norms[0, :workers]

        def first_copy(half, along, across, group):
            here = rows_of(half, along, across, group)
            at_start = pl.multiple_of(turned(at[1 - half], across) * block + group * sub, sub)
            return send(
                local.at[here], first.at[step, half, along - 1, pl.ds(at_start, sub)],
                first_send.at[half, along - 1, across, group], first_recv.at[step, half, along - 1, across, group],
                device(half, along, 0),
            )

        def spread(across, group):
            for along in reach + (0,):
                for half in range(2):
                    weigh(step, rows_of(half, along, across, group).start, whole)
            for along in reach:
                for half in range(2):
                    first_copy(half, along, across, group).start()

        def spread_far(i, carry):
            spread(1 + lax.rem(i + 1, SIDE - 1), lax.div(i, SIDE - 1))
            return carry

        def spread_near(i, carry):
            spread(0, i)
            return carry

        lax.fori_loop(0, (SIDE - 1) * GROUPS, spread_far, 0)
        lax.fori_loop(0, GROUPS, spread_near, 0)

        def second_copy(half, across, group):
            return send(
                second_out.at[half, across - 1, group], second.at[step, half, across - 1, group],
                second_send.at[half, across - 1, group], second_recv.at[step, half, across - 1, group],
                device(half, 0, across),
            )

        def summed(half, across, group):
            at_start = pl.multiple_of(turned(at[1 - half], across) * block + group * sub, sub)
            total = local[rows_of(half, 0, across, group), :]
            for along in reach:
                first_copy(half, along, across, group).wait_recv()
                total = total + first[step, half, along - 1, pl.ds(at_start, sub), :]
            return total

        def third_copy(half, across, group):
            here = rows_of(half, 0, 0, group)
            return send(
                value.at[step + 1, here], value.at[step + 1, here],
                third_send.at[half, across - 1, group], third_recv.at[step, half, across - 1, group],
                device(half, 0, across),
            )

        def fourth_copy(half, along, across, group):
            here = rows_of(half, 0, SIDE - across, group)
            return send(
                value.at[step + 1, here], value.at[step + 1, here],
                fourth_send.at[half, along - 1, across, group], fourth_recv.at[step, half, along - 1, across, group],
                device(half, along, 0),
            )

        for group in range(GROUPS):
            for across in FAR:
                for half in range(2):
                    second_out[half, across - 1, group] = summed(half, across, group)
                    second_copy(half, across, group).start()

        for group in range(GROUPS):
            for half in range(2):
                here = rows_of(half, 0, 0, group)
                total = summed(half, 0, group)
                for across in range(1, SIDE):
                    second_copy(half, across, group).wait_recv()
                    total = total + second[step, half, across - 1, group]
                value[step + 1, here, :] = value[step, here, :] + total / workers_all
                for across in reach:
                    third_copy(half, across, group).start()
                for along in reach:
                    fourth_copy(half, along, 0, group).start()

        totals = (zero, zero)

        def taken(half, along, across, group, totals):
            if step == ITERS - 1:
                return totals
            return squares_of(step + 1, rows_of(half, along, across, group).start, sub, totals)

        for group in range(GROUPS):
            for half in range(2):
                totals = taken(half, 0, 0, group, totals)
        for group in range(GROUPS):
            for across in (1, 3, 2):
                for half in range(2):
                    third_copy(half, across, group).wait_recv()
                    for along in reach:
                        fourth_copy(half, along, across, group).start()
                    totals = taken(half, 0, SIDE - across, group, totals)
        for group in range(GROUPS):
            for across in (0, 1, 3, 2):
                for along in (2, 1, 3):
                    for half in range(2):
                        fourth_copy(half, along, across, group).wait_recv()
                        totals = taken(half, SIDE - along, SIDE - across, group, totals)

        pending += [
            copy
            for group in range(GROUPS)
            for half in range(2)
            for copy in [
                make(half, along, across, group)
                for make in (first_copy, fourth_copy) for along in range(1, SIDE) for across in range(SIDE)
            ] + [make(half, across, group) for make in (second_copy, third_copy) for across in range(1, SIDE)]
        ]

    for copy in pending:
        copy.wait_send()
    out_ref[...] = value[ITERS]


def write_out(center_ref, norms_ref, center_out, norms_out, sem):
    copies = (
        pltpu.make_async_copy(center_ref, center_out, sem.at[0]),
        pltpu.make_async_copy(norms_ref, norms_out, sem.at[1]),
    )
    for copy in copies:
        copy.start()
    for copy in copies:
        copy.wait()


def shards(gradients, center, outside_sq, radius):
    workers, length = gradients.shape
    rows = length // LANES
    peers = lax.axis_size("mp")
    workers_all = workers * lax.axis_size("worker")
    root_total = float(length * peers) ** 0.5
    half_rows = rows // 2
    block = half_rows // (SIDE * SIDE)
    chunk = block * SIDE
    sub = block // GROUPS

    def body(*refs):
        kernel(float(workers_all), root_total, peers, *refs)

    dma = pltpu.SemaphoreType.DMA
    center_out, norms = pl.pallas_call(
        body,
        out_shape=(
            jax.ShapeDtypeStruct((rows, LANES), jnp.float32),
            jax.ShapeDtypeStruct((workers,), jnp.float32),
        ),
        in_specs=[
            pl.BlockSpec(memory_space=pltpu.HBM),
            pl.BlockSpec(memory_space=pltpu.HBM),
            pl.BlockSpec(memory_space=pltpu.HBM),
            pl.BlockSpec(memory_space=pltpu.HBM),
        ],
        out_specs=(pl.BlockSpec(memory_space=pltpu.VMEM), pl.BlockSpec(memory_space=pltpu.VMEM)),
        scratch_shapes=[
            pltpu.SMEM((ITERS,), jnp.float32),
            pltpu.VMEM((ITERS, workers), jnp.float32),
            pltpu.VMEM((workers, length), jnp.bfloat16),
            pltpu.VMEM((ITERS + 1, rows, LANES), jnp.float32),
            pltpu.VMEM((rows, LANES), jnp.float32),
            pltpu.VMEM((ITERS, 2, SIDE - 1, chunk, LANES), jnp.float32),
            pltpu.VMEM((ITERS, 2, SIDE - 1, GROUPS, sub, LANES), jnp.float32),
            pltpu.VMEM((2, SIDE - 1, GROUPS, sub, LANES), jnp.float32),
            pltpu.VMEM((ITERS, peers, LANES), jnp.float32),
            pltpu.VMEM((2 * workers, 2 * LANES), jnp.bfloat16),
            dma((2,)),
            dma((LOADS,)),
            dma((LOADS,)),
            dma((ITERS, peers - 1)),
            dma((ITERS, peers - 1)),
            dma((2, SIDE - 1, SIDE, GROUPS)),
            dma((ITERS, 2, SIDE - 1, SIDE, GROUPS)),
            dma((2, SIDE - 1, GROUPS)),
            dma((ITERS, 2, SIDE - 1, GROUPS)),
            dma((2, SIDE - 1, GROUPS)),
            dma((ITERS, 2, SIDE - 1, GROUPS)),
            dma((2, SIDE - 1, SIDE, GROUPS)),
            dma((ITERS, 2, SIDE - 1, SIDE, GROUPS)),
        ],
        compiler_params=pltpu.CompilerParams(
            collective_id=0, has_side_effects=True, vmem_limit_bytes=48 * 1024 * 1024
        ),
    )(*(
        pltpu.with_memory_space_constraint(value, pltpu.HBM)
        for value in (radius, gradients, center.reshape(rows, LANES), outside_sq)
    ))
    center_out, norms = pl.pallas_call(
        write_out,
        out_shape=(
            jax.ShapeDtypeStruct((rows, LANES), jnp.float32),
            jax.ShapeDtypeStruct((workers,), jnp.float32),
        ),
        in_specs=[pl.BlockSpec(memory_space=pl.ANY)] * 2,
        out_specs=(pl.BlockSpec(memory_space=pltpu.HBM),) * 2,
        scratch_shapes=[dma((2,))],
        compiler_params=pltpu.CompilerParams(vmem_limit_bytes=1024 * 1024),
    )(center_out, norms)
    return center_out.reshape(length), norms


def solution(mesh):
    placed = (P("worker", "mp"), P("mp"), P(None, "worker"), P())
    return jax.shard_map(
        shards, mesh=mesh, in_specs=placed, out_specs=(P("mp"), P("worker")), check_vma=False
    )
```
